8 devices in a mesh: dp: 1 (over z), a: 2 (over y), b: 4 (over x, core).
Axes of the slice: x: 2, y: 2, z: 1, core: 2. Of those that a mesh axis runs over, the one named last changes fastest.
Arguments:
- x: bfloat16 [2048, 12288], P('dp', ('a', 'b'))
- w_gate: bfloat16 [12288, 28672], P('a', 'b')
- w_up: bfloat16 [12288, 28672], P('a', 'b')
- w_down: bfloat16 [28672, 12288], P('b', 'a')
Outputs:
- output: bfloat16 [2048, 12288], P('dp', ('a', 'b'))
All inputs are finite; a program needn't handle non-finite values.
Results may differ from the reference program's by a relative error of at most 0.016.
Values are sent between devices in bfloat16 or wider.
A program may use at most 2 GiB of HBM per device.

```python
import jax
import jax.numpy as jnp

ROWS = 2048
D = 12288
FF = 28672


def setup_inputs(seed: int = 0, part: int = 0) -> dict:
    kx, kg, ku, kd = jax.random.split(jax.random.key(seed), 4)
    drawn = {
        "x": jax.random.normal(jax.random.fold_in(kx, part), (ROWS, D), jnp.float32),
        "w_gate": jax.random.normal(kg, (D, FF), jnp.float32) * D**-0.5,
        "w_up": jax.random.normal(ku, (D, FF), jnp.float32) * D**-0.5,
        "w_down": jax.random.normal(kd, (FF, D), jnp.float32) * FF**-0.5,
    }
    return {k: v.astype(jnp.bfloat16) for k, v in drawn.items()}


def reference(x, w_gate, w_up, w_down):
    gate = jnp.dot(x, w_gate, preferred_element_type=jnp.float32)
    up = jnp.dot(x, w_up, preferred_element_type=jnp.float32)
    hidden = (jax.nn.silu(gate) * up).astype(jnp.bfloat16)
    return jnp.dot(hidden, w_down, preferred_element_type=jnp.float32).astype(jnp.bfloat16)
```

```python
import jax
import jax.numpy as jnp
from jax import lax
from jax.sharding import PartitionSpec as P

HALVES = (256, 256, 256, 256)


def solution(mesh):
    na, nb = mesh.shape["a"], mesh.shape["b"]
    swap = [(0, 1), (1, 0)]

    def dot(p, q):
        return jnp.dot(p, q, preferred_element_type=jnp.float32)

    def body(x, w_gate, w_up, w_down):
        me = lax.axis_index("a")
        y = jnp.zeros((x.shape[0], w_down.shape[1] // nb), jnp.bfloat16)
        start = 0
        for rows in HALVES:
            mine = start + me * rows
            theirs = start + (1 - me) * rows
            start += 2 * rows
            xt = lax.all_gather(lax.dynamic_slice_in_dim(x, theirs, rows), "b", axis=1, tiled=True)
            gt = lax.ppermute(dot(xt, w_gate).astype(jnp.bfloat16), "a", swap)
            ut = lax.ppermute(dot(xt, w_up).astype(jnp.bfloat16), "a", swap)
            xm = lax.all_gather(lax.dynamic_slice_in_dim(x, mine, rows), "b", axis=1, tiled=True)
            gate = dot(xm, w_gate) + gt.astype(jnp.float32)
            up = dot(xm, w_up) + ut.astype(jnp.float32)
            hm = (jax.nn.silu(gate) * up).astype(jnp.bfloat16)
            ht = lax.ppermute(hm, "a", swap)
            for h, at in ((hm, mine), (ht, theirs)):
                part = dot(h, w_down).astype(jnp.bfloat16)
                out = lax.psum_scatter(part, "b", scatter_dimension=1, tiled=True)
                y = lax.dynamic_update_slice_in_dim(y, out, at, 0)
        return y

    return jax.shard_map(
        body,
        mesh=mesh,
        in_specs=(P("dp", ("a", "b")), P("a", "b"), P("a", "b"), P("b", "a")),
        out_specs=P("dp", ("a", "b")),
        check_vma=False,
    )
```

```python
import jax
import jax.numpy as jnp
from jax import lax
from jax.experimental import pallas as pl
from jax.experimental.pallas import tpu as pltpu
from jax.sharding import PartitionSpec as P

MESH = pl.DeviceIdType.MESH
BF16, F32 = jnp.bfloat16, jnp.float32

HALVES = (128, 448, 288, 160)
TN = 512
HT = TN // 2
NW = 5
RB = 32
ORDER = ("T0", "T1", "T2", "T3", "M0", "M1", "m0", "m1", "M2", "m2", "M3", "m3", "t0", "t1", "t2", "t3")


def solution(mesh):
    def body(x, w_gate, w_up, w_down):
        rows, dx = x.shape
        dk, ff = w_gate.shape
        dn = w_down.shape[1]
        steps, dsteps, groups = ff // HT, dn // TN, ff // TN
        per = dx // TN
        chunks, top = len(HALVES), max(HALVES)
        starts = [2 * sum(HALVES[:c]) for c in range(chunks)]
        plan = [(o[0], int(o[1])) for o in ORDER]
        jobs = [o for o in plan if o[0] in "tm"]
        tiles = [steps if kind in "TM" else dsteps for kind, _ in plan]
        base = [sum(tiles[:i]) for i in range(len(plan))]

        def kernel(x_ref, wg_ref, wu_ref, wd_ref, out_ref, xg_ref, *refs):
            ssend, srecv, hmine, htheirs = (refs[i * chunks : (i + 1) * chunks] for i in range(4))
            yrecv = refs[4 * chunks : 4 * chunks + len(jobs)]
            (lhs, w, gu, so, si, ho, ysend, ystash, yin, yout,
             wsem, lsem, osem, isem, ysem, yosem,
             fw_sem, xs_sem, xr_sem, ss_sem, sr_sem, hs_sem, hr_sem, ys_sem, yr_sem) = refs[4 * chunks + len(jobs) :]
            a, b = lax.axis_index("a"), lax.axis_index("b")
            other = 1 - a
            chip, core = b // 2, lax.rem(b, 2)

            def mate(g):
                flip_chip = 1 - g // 2
                flip_core = lax.rem((g + 1) // 2, 2)
                return 2 * (chip + flip_chip * (1 - 2 * chip)) + core + flip_core * (1 - 2 * core)

            mates = [mate(jnp.int32(g)) for g in range(3)]

            def row(c, mine):
                return pl.multiple_of(starts[c] + (a if mine else other) * HALVES[c], RB)

            def columns(of):
                return pl.ds(pl.multiple_of(of * dx, 128), dx)

            def gate_up_weights(j, slot):
                at = pl.ds(pl.multiple_of(j * HT, HT), HT)
                return (
                    pltpu.make_async_copy(wg_ref.at[:, at], w.at[slot, :dk, :HT], wsem.at[0, slot]),
                    pltpu.make_async_copy(wu_ref.at[:, at], w.at[slot, :dk, HT:], wsem.at[1, slot]),
                )

            def down_weights(j, slot):
                tile = mate(j // per) * per + lax.rem(j, per)
                at = pl.ds(pl.multiple_of(tile * TN, TN), TN)
                return (pltpu.make_async_copy(wd_ref.at[:, at], w.at[slot], wsem.at[0, slot]),)

            def weights(i, j, slot):
                return (gate_up_weights if plan[i][0] in "TM" else down_weights)(j, slot)

            def prefetch(i, j):
                ahead = j + NW - 1
                slot = lax.rem(base[i] + ahead, NW)

                @pl.when(ahead < tiles[i])
                def _():
                    for copy in weights(i, ahead, slot):
                        copy.start()

                if i + 1 < len(plan):
                    @pl.when(ahead >= tiles[i])
                    def _():
                        for copy in weights(i + 1, ahead - tiles[i], slot):
                            copy.start()

            for first in range(NW - 1):
                for copy in weights(0, jnp.int32(first), first):
                    copy.start()

            barrier = pltpu.get_barrier_semaphore()
            for g in range(3):
                pl.semaphore_signal(barrier, inc=1, device_id={"b": mates[g]}, device_id_type=MESH)
            pl.semaphore_signal(barrier, inc=1, device_id={"a": other}, device_id_type=MESH)
            pl.semaphore_wait(barrier, 4)

            def gather(c, mine, g):
                at = pl.ds(row(c, mine), HALVES[c])
                return pltpu.make_async_remote_copy(
                    x_ref.at[at], xg_ref.at[g, at], xs_sem.at[g], xr_sem.at[g, c, int(mine)],
                    device_id={"b": mates[g]}, device_id_type=MESH,
                )

            def forward(c):
                at = pl.ds(row(c, False), HALVES[c])
                return pltpu.make_async_remote_copy(
                    xg_ref.at[0, at], xg_ref.at[1, at], fw_sem, xr_sem.at[1, c, 0],
                    device_id={"b": mates[2]}, device_id_type=MESH,
                )

            for kind, c in plan:
                if kind in "TM":
                    for g in range(3):
                        if (kind, c, g) != ("T", 0, 1):
                            gather(c, kind == "M", g).start()
            gather(0, False, 0).wait_recv()
            forward(0).start()

            def load_x(c, mine):
                r, at = HALVES[c], pl.ds(row(c, mine), HALVES[c])
                copies = [pltpu.make_async_copy(x_ref.at[at], lhs.at[:r, columns(b)], lsem.at[3])]
                copies[0].start()
                for g in (0, 2, 1):
                    if (c, mine, g) != (0, False, 0):
                        gather(c, mine, g).wait_recv()
                    copies.append(pltpu.make_async_copy(xg_ref.at[g, at], lhs.at[:r, columns(mates[g])], lsem.at[g]))
                    copies[-1].start()
                for copy in copies:
                    copy.wait()

            def send_partial(c, g):
                at = pl.ds(2 * g, 2)
                return pltpu.make_async_remote_copy(
                    ssend[c].at[at], srecv[c].at[at], ss_sem.at[c], sr_sem.at[c, g],
                    device_id={"a": other}, device_id_type=MESH,
                )

            def send_hidden(c, g):
                return pltpu.make_async_remote_copy(
                    hmine[c].at[g], htheirs[c].at[g], hs_sem.at[c], hr_sem.at[c, g],
                    device_id={"a": other}, device_id_type=MESH,
                )

            def gate_up(i, c, mine):
                r = HALVES[c]
                load_x(c, mine)
                send = send_hidden if mine else send_partial

                def partial_in(j, slot):
                    return pltpu.make_async_copy(srecv[c].at[j], si.at[slot, :r], isem.at[slot])

                def put(j):
                    slot = lax.rem(j, 2)
                    if mine:
                        at = pl.ds(pl.multiple_of(slot * HT, HT), HT)
                        return pltpu.make_async_copy(ho.at[slot, :r], hmine[c].at[j // 2, :, at], osem.at[slot])
                    return pltpu.make_async_copy(so.at[slot, :r], ssend[c].at[j], osem.at[slot])

                if mine:
                    send_partial(c, 0).wait_recv()
                    partial_in(0, 0).start()

                def step(j, carry):
                    slot, two = lax.rem(base[i] + j, NW), lax.rem(j, 2)
                    prefetch(i, j)
                    if mine:
                        @pl.when(j + 1 < steps)
                        def _():
                            @pl.when(two == 1)
                            def _():
                                send_partial(c, (j + 1) // 2).wait_recv()
                            partial_in(j + 1, 1 - two).start()
                    for copy in weights(i, j, slot):
                        copy.wait()
                    both = jnp.dot(lhs[:r, :dk], w[slot, :dk], preferred_element_type=F32)
                    if mine:
                        gu[:r] = both
                        partial_in(j, two).wait()

                        def block(n, carry):
                            at = pl.ds(pl.multiple_of(n * RB, RB), RB)
                            gate = gu[at, :HT] + si[two, at, :HT].astype(F32)
                            up = gu[at, HT:] + si[two, at, HT:].astype(F32)
                            ho[two, at] = (jax.nn.silu(gate) * up).astype(BF16)
                            return carry

                        lax.fori_loop(0, r // RB, block, 0)
                    else:
                        so[two, :r] = both.astype(BF16)

                    @pl.when(j > 0)
                    def _():
                        put(j - 1).wait()

                        @pl.when(two == 0)
                        def _():
                            send(c, j // 2 - 1).start()

                    put(j).start()
                    return carry

                lax.fori_loop(0, steps, step, 0)
                put(steps - 1).wait()
                send(c, groups - 1).start()

            def give(job, r, n):
                g = n // per
                return pltpu.make_async_remote_copy(
                    ysend.at[n, :r], yrecv[job].at[n], ys_sem.at[n], yr_sem.at[job, n],
                    device_id={"b": mate(g)}, device_id_type=MESH,
                )

            def each(count, f):
                def one(n, carry):
                    f(n)
                    return carry

                lax.fori_loop(0, count, one, 0)

            def finish(job):
                kind, c = jobs[job]
                r = HALVES[c]

                def take(n):
                    return pltpu.make_async_copy(yrecv[job].at[n], yin.at[n, :r], ysem.at[n])

                def arrive(n):
                    give(job, r, n).wait()
                    take(n).start()

                each(3 * per, arrive)
                each(3 * per, lambda n: take(n).wait())

                def block(n):
                    at = pl.ds(pl.multiple_of(n * RB, RB), RB)
                    for p in range(per):
                        cols = slice(p * TN, (p + 1) * TN)
                        total = ystash[at, cols]
                        for g in range(3):
                            total = total + yin[g * per + p, at].astype(F32)
                        yout[at, cols] = total.astype(BF16)

                each(r // RB, block)
                copy = pltpu.make_async_copy(yout.at[:r], out_ref.at[pl.ds(row(c, kind == "m"), r)], yosem)
                copy.start()
                copy.wait()

            def down_job(i, job, c, mine):
                r = HALVES[c]
                source = (hmine if mine else htheirs)[c]

                def hidden_in(g):
                    at = pl.ds(pl.multiple_of(g * TN, TN), TN)
                    return pltpu.make_async_copy(source.at[g], lhs.at[:r, at], lsem.at[0])

                def load(g):
                    if not mine:
                        send_hidden(c, g).wait_recv()
                    hidden_in(g).start()

                each(groups, load)
                each(groups, lambda g: hidden_in(g).wait())

                def compute(j):
                    slot = lax.rem(base[i] + j, NW)
                    prefetch(i, j)
                    for copy in weights(i, j, slot):
                        copy.wait()
                    gu[:r] = jnp.dot(lhs[:r], w[slot], preferred_element_type=F32)

                def part(j):
                    compute(j)
                    ysend[j, :r] = gu[:r].astype(BF16)
                    give(job, r, j).start()

                def own(j):
                    compute(j + 3 * per)
                    ystash[:r, pl.ds(pl.multiple_of(j * TN, TN), TN)] = gu[:r]

                if job:
                    finish(job - 1)
                each(3 * per, part)
                each(per, own)

            for i, (kind, c) in enumerate(plan):
                if kind in "TM":
                    gate_up(i, c, kind == "M")
                else:
                    down_job(i, jobs.index((kind, c)), c, kind == "m")
            finish(len(jobs) - 1)

            for c in range(chunks):
                pltpu.make_async_remote_copy(
                    ssend[c], srecv[c], ss_sem.at[c], sr_sem.at[c, 0], device_id={"a": other}, device_id_type=MESH
                ).wait_send()
                pltpu.make_async_remote_copy(
                    hmine[c], htheirs[c], hs_sem.at[c], hr_sem.at[c, 0], device_id={"a": other}, device_id_type=MESH
                ).wait_send()
            forward(0).wait_send()
            for g in range(3):
                sent = pl.ds(0, rows - HALVES[0] if g == 1 else rows)
                pltpu.make_async_remote_copy(
                    x_ref.at[sent], xg_ref.at[g, sent], xs_sem.at[g], xr_sem.at[g, 0, 0],
                    device_id={"b": mates[g]}, device_id_type=MESH,
                ).wait_send()

        def hbm(*shape):
            return jax.ShapeDtypeStruct(shape, BF16)

        outs = [hbm(rows, dx), hbm(3, rows, dx)]
        outs += [hbm(steps, r, TN) for r in HALVES] * 2
        outs += [hbm(groups, r, TN) for r in HALVES] * 2
        outs += [hbm(3 * per, HALVES[c], TN) for _, c in jobs]
        sem = pltpu.SemaphoreType.DMA
        result = pl.pallas_call(
            kernel,
            name="gated_mlp",
            out_shape=outs,
            in_specs=[pl.BlockSpec(memory_space=pl.ANY)] * 4,
            out_specs=[pl.BlockSpec(memory_space=pl.ANY)] * len(outs),
            scratch_shapes=[
                pltpu.VMEM((top, ff), BF16),
                pltpu.VMEM((NW, ff, TN), BF16),
                pltpu.VMEM((top, TN), F32),
                pltpu.VMEM((2, top, TN), BF16),
                pltpu.VMEM((2, top, TN), BF16),
                pltpu.VMEM((2, top, HT), BF16),
                pltpu.VMEM((3 * per, top, TN), BF16),
                pltpu.VMEM((top, dx), F32),
                pltpu.VMEM((3 * per, top, TN), BF16),
                pltpu.VMEM((top, dx), BF16),
                sem((2, NW)), sem((4,)), sem((2,)), sem((2,)), sem((3 * per,)), sem,
                sem, sem((3,)), sem((3, chunks, 2)),
                sem((chunks,)), sem((chunks, groups)),
                sem((chunks,)), sem((chunks, groups)),
                sem((3 * per,)), sem((len(jobs), 3 * per)),
            ],
            compiler_params=pltpu.CompilerParams(
                collective_id=0, has_side_effects=True, vmem_limit_bytes=67043328
            ),
        )(x, w_gate, w_up, w_down)
        return result[0]

    return jax.shard_map(
        body,
        mesh=mesh,
        in_specs=(P("dp", ("a", "b")), P("a", "b"), P("a", "b"), P("b", "a")),
        out_specs=P("dp", ("a", "b")),
        check_vma=False,
    )
```

```python
import jax
import jax.numpy as jnp
from jax import lax
from jax.experimental import pallas as pl
from jax.experimental.pallas import tpu as pltpu
from jax.sharding import PartitionSpec as P

MESH = pl.DeviceIdType.MESH
BF16, F32 = jnp.bfloat16, jnp.float32

HALVES = (128, 448, 304, 144)
TN = 512
HT = TN // 2
NW = 5
RB = 16
ORDER = ("T0", "T1", "T2", "T3", "M0", "M1", "m0", "m1", "M2", "m2", "M3", "m3", "t0", "t1", "t2", "t3")


def solution(mesh):
    def body(x, w_gate, w_up, w_down):
        rows, dx = x.shape
        dk, ff = w_gate.shape
        dn = w_down.shape[1]
        steps, dsteps, groups = ff // HT, dn // TN, ff // TN
        per = dx // TN
        chunks, top = len(HALVES), max(HALVES)
        starts = [2 * sum(HALVES[:c]) for c in range(chunks)]
        plan = [(o[0], int(o[1])) for o in ORDER]
        jobs = [o for o in plan if o[0] in "tm"]
        tiles = [steps if kind in "TM" else dsteps for kind, _ in plan]
        base = [sum(tiles[:i]) for i in range(len(plan))]

        def kernel(x_ref, wg_ref, wu_ref, wd_ref, out_ref, xg_ref, *refs):
            ssend, srecv, hmine, htheirs = (refs[i * chunks : (i + 1) * chunks] for i in range(4))
            yrecv = refs[4 * chunks : 4 * chunks + len(jobs)]
            (lhs, w, gu, so, si, ho, ysend, ystash, yin, yout,
             wsem, lsem, osem, isem, ysem, yosem,
             fw_sem, xs_sem, xr_sem, ss_sem, sr_sem, hs_sem, hr_sem, ys_sem, yr_sem) = refs[4 * chunks + len(jobs) :]
            a, b = lax.axis_index("a"), lax.axis_index("b")
            other = 1 - a
            chip, core = b // 2, lax.rem(b, 2)

            def mate(g):
                flip_chip = 1 - g // 2
                flip_core = lax.rem((g + 1) // 2, 2)
                return 2 * (chip + flip_chip * (1 - 2 * chip)) + core + flip_core * (1 - 2 * core)

            mates = [mate(jnp.int32(g)) for g in range(3)]

            def row(c, mine):
                return pl.multiple_of(starts[c] + (a if mine else other) * HALVES[c], RB)

            def columns(of):
                return pl.ds(pl.multiple_of(of * dx, 128), dx)

            def gate_up_weights(j, slot):
                at = pl.ds(pl.multiple_of(j * HT, HT), HT)
                return (
                    pltpu.make_async_copy(wg_ref.at[:, at], w.at[slot, :dk, :HT], wsem.at[0, slot]),
                    pltpu.make_async_copy(wu_ref.at[:, at], w.at[slot, :dk, HT:], wsem.at[1, slot]),
                )

            def down_weights(j, slot):
                tile = mate(j // per) * per + lax.rem(j, per)
                at = pl.ds(pl.multiple_of(tile * TN, TN), TN)
                return (pltpu.make_async_copy(wd_ref.at[:, at], w.at[slot], wsem.at[0, slot]),)

            def weights(i, j, slot):
                return (gate_up_weights if plan[i][0] in "TM" else down_weights)(j, slot)

            def prefetch(i, j):
                ahead = j + NW - 1
                slot = lax.rem(base[i] + ahead, NW)

                @pl.when(ahead < tiles[i])
                def _():
                    for copy in weights(i, ahead, slot):
                        copy.start()

                if i + 1 < len(plan):
                    @pl.when(ahead >= tiles[i])
                    def _():
                        for copy in weights(i + 1, ahead - tiles[i], slot):
                            copy.start()

            for first in range(NW - 1):
                for copy in weights(0, jnp.int32(first), first):
                    copy.start()

            barrier = pltpu.get_barrier_semaphore()
            for g in range(3):
                pl.semaphore_signal(barrier, inc=1, device_id={"b": mates[g]}, device_id_type=MESH)
            pl.semaphore_signal(barrier, inc=1, device_id={"a": other}, device_id_type=MESH)
            pl.semaphore_wait(barrier, 4)

            def gather(c, mine, g):
                at = pl.ds(row(c, mine), HALVES[c])
                return pltpu.make_async_remote_copy(
                    x_ref.at[at], xg_ref.at[g, at], xs_sem.at[g], xr_sem.at[g, c, int(mine)],
                    device_id={"b": mates[g]}, device_id_type=MESH,
                )

            def forward(c):
                at = pl.ds(row(c, False), HALVES[c])
                return pltpu.make_async_remote_copy(
                    xg_ref.at[0, at], xg_ref.at[1, at], fw_sem, xr_sem.at[1, c, 0],
                    device_id={"b": mates[2]}, device_id_type=MESH,
                )

            for kind, c in plan:
                if kind in "TM":
                    for g in range(3):
                        if (kind, c, g) != ("T", 0, 1):
                            gather(c, kind == "M", g).start()
            gather(0, False, 0).wait_recv()
            forward(0).start()

            def load_x(c, mine):
                r, at = HALVES[c], pl.ds(row(c, mine), HALVES[c])
                copies = [pltpu.make_async_copy(x_ref.at[at], lhs.at[:r, columns(b)], lsem.at[3])]
                copies[0].start()
                for g in (0, 2, 1):
                    if (c, mine, g) != (0, False, 0):
                        gather(c, mine, g).wait_recv()
                    copies.append(pltpu.make_async_copy(xg_ref.at[g, at], lhs.at[:r, columns(mates[g])], lsem.at[g]))
                    copies[-1].start()
                for copy in copies:
                    copy.wait()

            def send_partial(c, j):
                return pltpu.make_async_remote_copy(
                    ssend[c].at[j], srecv[c].at[j], ss_sem.at[c], sr_sem.at[c, j],
                    device_id={"a": other}, device_id_type=MESH,
                )

            def send_hidden(c, g):
                return pltpu.make_async_remote_copy(
                    hmine[c].at[g], htheirs[c].at[g], hs_sem.at[c], hr_sem.at[c, g],
                    device_id={"a": other}, device_id_type=MESH,
                )

            def gate_up(i, c, mine):
                r, early = HALVES[c], i == 0
                load_x(c, mine)

                def partial_in(j, slot):
                    return pltpu.make_async_copy(srecv[c].at[j], si.at[slot, :r], isem.at[slot])

                def put(j):
                    slot = lax.rem(j, 2)
                    if mine:
                        at = pl.ds(pl.multiple_of(slot * HT, HT), HT)
                        return pltpu.make_async_copy(ho.at[slot, :r], hmine[c].at[j // 2, :, at], osem.at[slot])
                    return pltpu.make_async_copy(so.at[slot, :r], ssend[c].at[j], osem.at[slot])

                if mine:
                    send_partial(c, 0).wait_recv()
                    partial_in(0, 0).start()

                def step(j, carry):
                    slot, two = lax.rem(base[i] + j, NW), lax.rem(j, 2)
                    prefetch(i, j)
                    if mine:
                        @pl.when(j + 1 < steps)
                        def _():
                            send_partial(c, j + 1).wait_recv()
                            partial_in(j + 1, 1 - two).start()
                    for copy in weights(i, j, slot):
                        copy.wait()
                    both = jnp.dot(lhs[:r, :dk], w[slot, :dk], preferred_element_type=F32)
                    if mine:
                        gu[:r] = both
                        partial_in(j, two).wait()

                        def block(n, carry):
                            at = pl.ds(pl.multiple_of(n * RB, RB), RB)
                            gate = gu[at, :HT] + si[two, at, :HT].astype(F32)
                            up = gu[at, HT:] + si[two, at, HT:].astype(F32)
                            ho[two, at] = (jax.nn.silu(gate) * up).astype(BF16)
                            return carry

                        lax.fori_loop(0, r // RB, block, 0)
                    else:
                        so[two, :r] = both.astype(BF16)

                    if early:
                        put(j).start()
                        put(j).wait()
                        send_partial(c, j).start()
                        return carry

                    @pl.when(j > 0)
                    def _():
                        put(j - 1).wait()
                        if mine:
                            @pl.when(two == 0)
                            def _():
                                send_hidden(c, j // 2 - 1).start()
                        else:
                            send_partial(c, j - 1).start()

                    put(j).start()
                    return carry

                lax.fori_loop(0, steps, step, 0)
                if not early:
                    put(steps - 1).wait()
                    if mine:
                        send_hidden(c, groups - 1).start()
                    else:
                        send_partial(c, steps - 1).start()

            def give(job, r, n):
                g = n // per
                return pltpu.make_async_remote_copy(
                    ysend.at[n, :r], yrecv[job].at[n], ys_sem.at[n], yr_sem.at[job, n],
                    device_id={"b": mate(g)}, device_id_type=MESH,
                )

            def each(count, f):
                def one(n, carry):
                    f(n)
                    return carry

                lax.fori_loop(0, count, one, 0)

            def put_out(job):
                kind, c = jobs[job]
                r = HALVES[c]
                return pltpu.make_async_copy(yout.at[:r], out_ref.at[pl.ds(row(c, kind == "m"), r)], yosem)

            def sent(job):
                each(3 * per, lambda n: give(job, HALVES[jobs[job][1]], n).wait_send())

            def finish(job):
                r = HALVES[jobs[job][1]]

                def take(n):
                    return pltpu.make_async_copy(yrecv[job].at[n], yin.at[n, :r], ysem.at[n])

                def arrive(n):
                    give(job, r, n).wait_recv()
                    take(n).start()

                each(3 * per, arrive)
                each(3 * per, lambda n: take(n).wait())

                if job:
                    put_out(job - 1).wait()

                def block(n):
                    at = pl.ds(pl.multiple_of(n * RB, RB), RB)
                    for p in range(per):
                        cols = slice(p * TN, (p + 1) * TN)
                        total = ystash[at, cols]
                        for g in range(3):
                            total = total + yin[g * per + p, at].astype(F32)
                        yout[at, cols] = total.astype(BF16)

                each(r // RB, block)
                put_out(job).start()

            def down_job(i, job, c, mine):
                r = HALVES[c]
                source = (hmine if mine else htheirs)[c]

                def hidden_in(g):
                    at = pl.ds(pl.multiple_of(g * TN, TN), TN)
                    return pltpu.make_async_copy(source.at[g], lhs.at[:r, at], lsem.at[0])

                def load(g):
                    if not mine:
                        send_hidden(c, g).wait_recv()
                    hidden_in(g).start()

                each(groups, load)
                each(groups, lambda g: hidden_in(g).wait())

                def compute(j):
                    slot = lax.rem(base[i] + j, NW)
                    prefetch(i, j)
                    for copy in weights(i, j, slot):
                        copy.wait()
                    gu[:r] = jnp.dot(lhs[:r], w[slot], preferred_element_type=F32)

                def part(j):
                    compute(j)
                    ysend[j, :r] = gu[:r].astype(BF16)
                    give(job, r, j).start()

                def own(j):
                    compute(j + 3 * per)
                    ystash[:r, pl.ds(pl.multiple_of(j * TN, TN), TN)] = gu[:r]

                if job:
                    sent(job - 1)
                each(3 * per, part)
                if job:
                    finish(job - 1)
                each(per, own)

            for i, (kind, c) in enumerate(plan):
                if kind in "TM":
                    gate_up(i, c, kind == "M")
                else:
                    down_job(i, jobs.index((kind, c)), c, kind == "m")
            finish(len(jobs) - 1)
            put_out(len(jobs) - 1).wait()
            sent(len(jobs) - 1)

            for c in range(chunks):
                pltpu.make_async_remote_copy(
                    ssend[c], srecv[c], ss_sem.at[c], sr_sem.at[c, 0], device_id={"a": other}, device_id_type=MESH
                ).wait_send()
                pltpu.make_async_remote_copy(
                    hmine[c], htheirs[c], hs_sem.at[c], hr_sem.at[c, 0], device_id={"a": other}, device_id_type=MESH
                ).wait_send()
            forward(0).wait_send()
            for g in range(3):
                part = pl.ds(0, rows - HALVES[0] if g == 1 else rows)
                pltpu.make_async_remote_copy(
                    x_ref.at[part], xg_ref.at[g, part], xs_sem.at[g], xr_sem.at[g, 0, 0],
                    device_id={"b": mates[g]}, device_id_type=MESH,
                ).wait_send()

        def hbm(*shape):
            return jax.ShapeDtypeStruct(shape, BF16)

        outs = [hbm(rows, dx), hbm(3, rows, dx)]
        outs += [hbm(steps, r, TN) for r in HALVES] * 2
        outs += [hbm(groups, r, TN) for r in HALVES] * 2
        outs += [hbm(3 * per, HALVES[c], TN) for _, c in jobs]
        sem = pltpu.SemaphoreType.DMA
        result = pl.pallas_call(
            kernel,
            name="gated_mlp",
            out_shape=outs,
            in_specs=[pl.BlockSpec(memory_space=pl.ANY)] * 4,
            out_specs=[pl.BlockSpec(memory_space=pl.ANY)] * len(outs),
            scratch_shapes=[
                pltpu.VMEM((top, ff), BF16),
                pltpu.VMEM((NW, ff, TN), BF16),
                pltpu.VMEM((top, TN), F32),
                pltpu.VMEM((2, top, TN), BF16),
                pltpu.VMEM((2, top, TN), BF16),
                pltpu.VMEM((2, top, HT), BF16),
                pltpu.VMEM((3 * per, top, TN), BF16),
                pltpu.VMEM((top, dx), F32),
                pltpu.VMEM((3 * per, top, TN), BF16),
                pltpu.VMEM((top, dx), BF16),
                sem((2, NW)), sem((4,)), sem((2,)), sem((2,)), sem((3 * per,)), sem,
                sem, sem((3,)), sem((3, chunks, 2)),
                sem((chunks,)), sem((chunks, steps)),
                sem((chunks,)), sem((chunks, groups)),
                sem((3 * per,)), sem((len(jobs), 3 * per)),
            ],
            compiler_params=pltpu.CompilerParams(
                collective_id=0, has_side_effects=True, vmem_limit_bytes=67043328
            ),
        )(x, w_gate, w_up, w_down)
        return result[0]

    return jax.shard_map(
        body,
        mesh=mesh,
        in_specs=(P("dp", ("a", "b")), P("a", "b"), P("a", "b"), P("b", "a")),
        out_specs=P("dp", ("a", "b")),
        check_vma=False,
    )
```
